32 devices in a mesh: section: 4 (over z), rows: 8 (over y, x, core).
Axes of the slice: x: 2, y: 2, z: 4, core: 2. Of those that a mesh axis runs over, the one named last changes fastest.
Arguments:
- features: bfloat16 [1024, 1536], P('rows'), may hold values from -6 to 6
- ages: int32 [1024], P('rows'), may hold values from 0 to 15
- age_table: bfloat16 [16, 1536], replicated, may hold values from -3 to 3
- returns: float32 [1024], P('rows'), may hold values from -6 to 6
- owners: int32 [1024, 1], P('rows'), may hold values from 0 to 7; in each aligned block of 128 rows (0 to 127, 128 to 255, ...) at most 32 rows name the same one
- slots: int32 [1024], P('rows'), may hold values from 0 to 4095
- norm_gain: float32 [4, 1536], P('section'), may hold values from 0.1 to 1.9
- w_gate: bfloat16 [4, 1536, 8960], P('section', None, 'rows'), may hold values from -0.15625 to 0.15625
- w_up: bfloat16 [4, 1536, 8960], P('section', None, 'rows'), may hold values from -0.15625 to 0.15625
- w_down: bfloat16 [4, 8960, 1536], P('section', 'rows'), may hold values from -0.0625 to 0.0625
- final_gain: float32 [1536], replicated, may hold values from 0.1 to 1.9
- reward_head: float32 [1536], replicated, may hold values from -0.15625 to 0.15625
- old_priority: float32 [32768], P('rows'), may hold values from 0.05 to 2
Outputs:
- rewards: float32 [1024], P(('rows', 'section'))
- weights: float32 [32768], P(('rows', 'section'))
The draws below stay inside these ranges and needn't reach their ends.
Inputs may be any that keep to these rules, and one draw needn't show every extreme that they name: `owners`: among the rows of one device at most 32 name the same owner; in every draw some owner is named by exactly 32 rows of some device.
All inputs are finite; a program needn't handle non-finite values.
Results may differ from the reference program's by a relative error of at most 0.04.
Values may be sent and summed in bfloat16 or wider, within the bound.
A program may use at most 64 MiB of HBM per device.

```python
import math
import jax
import jax.numpy as jnp
import numpy as np
from jax import lax

D = 1536
FF = 8960
AGES = 16
CAP = 32
ROWS_DEV = 128
BUF_DEV = 4096
LAYERS = 4
ROWS = 1024
OWNERS = 8
BUF = 32768


def set_ends(result, own_key, low, high):
    longest = result.shape.index(max(result.shape))
    spots = []
    for shift in (0, 1):
        where = [jax.random.randint(jax.random.fold_in(own_key, axis), (), 0, length) for axis, length in enumerate(result.shape)]
        where[longest] = (where[longest] + shift) % result.shape[longest]
        spots.append(tuple(where))
    return result.at[spots[0]].set(low).at[spots[1]].set(high)


def shard_levels(key, extent, cuts, least, high):
    loudness, own = 1.0, jax.random.fold_in(key, 6)
    for axis_at, parts in cuts:
        steps = jnp.exp(jax.random.uniform(jax.random.fold_in(own, axis_at), (parts,), jnp.float32, least / len(cuts), high / len(cuts)))
        loudness = loudness * jnp.repeat(steps, extent[axis_at] // parts).reshape([-1 if axis == axis_at else 1 for axis in range(len(extent))])
    return loudness


def assign_block(stream_key, own, number, rows, amount, top, reach, slope):
    order = jax.random.permutation(stream_key, amount)
    packed, usual = portions_of(amount, rows * top, reach, slope, True), portions_of(amount, rows * top, reach, slope, False)
    places = jnp.arange(amount)

    def named(lengths, rotation):
        used = int((lengths > 0).sum())
        fixed = max(1, used // 4)
        passed = fixed + (places - fixed + rotation * (used - fixed)) % max(1, amount - fixed)
        return jnp.zeros((amount,), jnp.int32).at[order[jnp.where(places < fixed, places, passed)]].set(jnp.asarray(lengths, jnp.int32))

    lengths = jnp.where(number % 4 == 0, named(packed, number // 4), named(usual, number - number // 4 - 1))
    mixed = jax.random.permutation(jax.random.fold_in(own, 3), amount)
    giver, sink = mixed[0:amount // 2 * 2:2], mixed[1:amount // 2 * 2:2]
    margin = jnp.minimum(lengths[giver] - 1, reach - lengths[sink]) // 2
    margin = jnp.where((giver == order[0]) | (sink == order[0]) | (lengths[sink] == 0), 0, jnp.maximum(margin, 0))
    passed = jax.random.randint(jax.random.fold_in(own, 4), (amount // 2,), 0, 1 << 20) % (margin + 1)
    lengths = lengths.at[giver].add(-passed).at[sink].add(passed)
    items = jnp.searchsorted(jnp.cumsum(lengths), jnp.arange(rows * top), side="right").astype(jnp.int32)
    grid = items.reshape(top, rows).T
    grid = grid[jax.random.permutation(jax.random.fold_in(own, 1), rows)]
    rotation = jax.random.randint(jax.random.fold_in(own, 2), (rows, 1), 0, top)
    return jnp.take_along_axis(grid, (jnp.arange(top)[None, :] + rotation) % top, axis=1)


def portions_of(count, total, reach, skew, full):
    loads = [(1 << 20) // math.isqrt(grade ** skew) + 1 for grade in range(1, count + 1)]
    largest = reach if full else min(reach, max(-(-total // count), total * loads[0] // sum(loads)))
    least = 1 if total - largest >= count - 1 else 0
    counts, surplus = [largest] + [least] * (count - 1), total - largest - least * (count - 1)
    while surplus > 0:
        candidates = [i for i in range(1, count) if counts[i] < largest] or [i for i in range(1, count) if counts[i] < reach]
        whole, budget = sum([loads[i] for i in candidates]), surplus
        for i in candidates:
            more = min(reach - counts[i], max(1, budget * loads[i] // whole), surplus)
            counts[i] = counts[i] + more
            surplus = surplus - more
    return np.array(counts)


def normal_values(key, dims, scale, most, split=(), dtype=jnp.bfloat16):
    result = scale * jax.random.normal(key, dims, jnp.float32)
    if split:
        result = result * shard_levels(key, dims, split, -0.22, 0.18)
    return jnp.clip(result, -most, most).astype(dtype)


def setup_inputs(seed: int = 0) -> dict:
    arg_keys = jax.random.split(jax.random.key(seed), 14)
    features = normal_values(arg_keys[0], (ROWS, D), 1.0, 6.0, ((0, 8),))
    ages = set_ends(jax.random.randint(arg_keys[1], (ROWS,), 0, AGES), jax.random.fold_in(arg_keys[1], 1), 0, AGES - 1).astype(jnp.int32)
    age_table = normal_values(arg_keys[2], (AGES, D), 0.5, 3.0)
    returns = normal_values(arg_keys[3], (ROWS,), 1.0, 6.0, ((0, 8),), jnp.float32)
    owners_keys = jax.random.split(jax.random.fold_in(arg_keys[4], 1), ROWS // ROWS_DEV)
    owners_turns = jax.random.permutation(jax.random.fold_in(arg_keys[4], 3), ROWS // ROWS_DEV)
    owners = jax.vmap(lambda own, number: assign_block(jax.random.fold_in(arg_keys[4], 2), own, number, ROWS_DEV, OWNERS, 1, CAP, 2))(owners_keys, owners_turns).reshape((ROWS, 1))
    slots = set_ends(jax.random.randint(arg_keys[5], (ROWS,), 0, BUF_DEV), jax.random.fold_in(arg_keys[5], 1), 0, BUF_DEV - 1).astype(jnp.int32)
    norm_gain = jnp.clip(1.0 + 0.18 * jax.random.normal(arg_keys[6], (LAYERS, D), jnp.float32), 0.1, 1.9)
    w_gate = normal_values(arg_keys[7], (LAYERS, D, FF), D ** -0.5, 0.15625, ((0, 4), (2, 8)))
    w_up = normal_values(arg_keys[8], (LAYERS, D, FF), D ** -0.5, 0.15625, ((0, 4), (2, 8)))
    w_down = normal_values(arg_keys[9], (LAYERS, FF, D), FF ** -0.5, 0.0625, ((0, 4), (1, 8)))
    final_gain = jnp.clip(1.0 + 0.18 * jax.random.normal(arg_keys[10], (D,), jnp.float32), 0.1, 1.9)
    reward_head = normal_values(arg_keys[11], (D,), D ** -0.5, 0.15625, (), jnp.float32)
    old_priority = jnp.clip(jnp.exp(math.log(2.0) - 3.6888794 * jax.random.uniform(arg_keys[12], (BUF,), jnp.float32) ** shard_levels(arg_keys[12], (BUF,), ((0, 8),), -0.2, 0.2)), 0.05, 2.0)
    return dict(features=features, ages=ages, age_table=age_table, returns=returns, owners=owners, slots=slots, norm_gain=norm_gain, w_gate=w_gate, w_up=w_up, w_down=w_down, final_gain=final_gain, reward_head=reward_head, old_priority=old_priority)


def scaled_norm(values, gain):
    return values * lax.rsqrt(lax.optimization_barrier(jnp.mean(values * values, axis=-1, keepdims=True)) + 1e-06) * gain

def reference(features, ages, age_table, returns, owners, slots, norm_gain, w_gate, w_up, w_down, final_gain, reward_head, old_priority):
    onehot = (ages[:, None] == jnp.arange(AGES)[None, :]).astype(jnp.bfloat16)
    state = (features.astype(jnp.float32) + jnp.dot(onehot, age_table, preferred_element_type=jnp.float32)).astype(jnp.bfloat16)
    for layer in range(LAYERS):
        wide = state.astype(jnp.float32)
        normed = scaled_norm(wide, norm_gain[layer]).astype(jnp.bfloat16)
        gate = jnp.dot(normed, w_gate[layer], preferred_element_type=jnp.float32)
        upper = jnp.dot(normed, w_up[layer], preferred_element_type=jnp.float32)
        hidden = (jax.nn.silu(gate) * upper).astype(jnp.bfloat16)
        state = (wide + jnp.dot(hidden, w_down[layer], preferred_element_type=jnp.float32)).astype(jnp.bfloat16)
    finished = scaled_norm(state.astype(jnp.float32), final_gain)
    rewards = lax.optimization_barrier(jnp.sum(finished * reward_head, axis=-1))
    priority = jnp.exp(0.6 * jnp.log(jnp.abs(rewards - returns) + 0.05))
    target = (owners[:, 0] * BUF_DEV + slots).astype(jnp.int32)
    largest = jax.ops.segment_max(priority, target, num_segments=BUF)
    counted = jax.ops.segment_sum(jnp.ones_like(priority), target, num_segments=BUF)
    refreshed = jnp.where(counted > 0, largest, old_priority)
    weights = refreshed * (BUF / jnp.sum(refreshed))
    return (rewards, weights)
```

```python
import functools

import jax
import jax.numpy as jnp
from jax import lax
from jax.experimental import pallas as pl
from jax.experimental.pallas import tpu as pltpu
from jax.sharding import PartitionSpec as P

MICRO = 8
MESH = pl.DeviceIdType.MESH
LANES = 128


def chunks(total, size):
    return [(at, min(size, total - at)) for at in range(0, total, size)]


def remote(src, dst, send_sem, recv_sem, where):
    return pltpu.make_async_remote_copy(
        src_ref=src, dst_ref=dst, send_sem=send_sem, recv_sem=recv_sem,
        device_id=where, device_id_type=MESH,
    )


def kernel(
    sections, groups,
    features, ages, age_table, returns, target, gain, w_gate, w_up, w_down,
    final_gain, head, old,
    rewards_out, weights_out,
    wg, wu, wd, x_in, x_out, gathered, hidden, part, part_in, paired, paired_in,
    reward_cols, marks, marks_wide, result, prio_wide, refreshed, sums,
    w_sem,
    ag_send, ag_recv, fw_send, fw_recv, pr_send, pr_recv, rs_send, rs_recv, z_send, z_recv,
    mk_send, mk_recv, up_send, up_recv, rw_send, rw_recv, sm_send, sm_recv,
):
    sec = lax.axis_index("section")
    me = lax.axis_index("rows")
    chips = groups // 2
    chip, core = me // 2, lax.rem(me, 2)
    other = 1 - core
    sibling = chip * 2 + other
    block, width = x_in.shape[1], x_in.shape[2]
    rows = x_in.shape[0] * block
    ff = hidden.shape[1]
    last = sections - 1

    loads = [
        pltpu.make_async_copy(w_gate, wg, w_sem.at[0]),
        pltpu.make_async_copy(w_up, wu, w_sem.at[1]),
        pltpu.make_async_copy(w_down, wd, w_sem.at[2]),
    ]
    for load in loads:
        load.start()

    barrier = pltpu.get_barrier_semaphore()
    for j in range(1, groups):
        pl.semaphore_signal(barrier, inc=1, device_id={"rows": lax.rem(me + j, groups)}, device_id_type=MESH)
    for j in range(1, sections):
        pl.semaphore_signal(barrier, inc=1, device_id={"section": lax.rem(sec + j, sections)}, device_id_type=MESH)

    marks[me] = target[...]

    @pl.when(sec == 0)
    def _():
        tall = jnp.transpose(jnp.broadcast_to(ages[...].astype(jnp.float32), (LANES, rows)))
        buckets = age_table.shape[0]
        onehot = (
            tall[:, :buckets] == lax.broadcasted_iota(jnp.int32, (rows, buckets), 1).astype(jnp.float32)
        ).astype(jnp.float32).astype(jnp.bfloat16)
        for at, size in chunks(width, 512):
            entry = features[:, at:at + size].astype(jnp.float32) + jnp.dot(
                onehot, age_table[:, at:at + size], preferred_element_type=jnp.float32
            )
            x_in[:, :, at:at + size] = entry.astype(jnp.bfloat16).reshape(MICRO, block, size)

    pl.semaphore_wait(barrier, groups - 1 + sections - 1)

    def to_group(ref, send, recv, j):
        return remote(ref.at[me], ref.at[me], send.at[j], recv.at[j], {"rows": lax.rem(me + j, groups)})

    def from_group(ref, send, recv, j):
        spot = ref.at[lax.rem(me + groups - j, groups)]
        return remote(spot, spot, send.at[j], recv.at[j], {"rows": lax.rem(me + j, groups)})

    def peer(j):
        return {"rows": lax.rem(chip + j, chips) * 2 + core}

    def ag_copy(m, j, spot):
        block_ref = gathered.at[m, core, spot]
        return remote(block_ref, block_ref, ag_send.at[m, j - 1], ag_recv.at[m, j - 1], peer(j))

    def fw_copy(m, half):
        half_ref = gathered.at[m, half]
        return remote(half_ref, half_ref, fw_send.at[m], fw_recv.at[m], {"rows": sibling})

    def pr_copy(m):
        return remote(part.at[m, other], part_in.at[m], pr_send.at[m], pr_recv.at[m], {"rows": sibling})

    def rs_copy(m, j):
        return remote(
            paired.at[m, lax.rem(chip + j, chips)], paired_in.at[m, j - 1],
            rs_send.at[m, j - 1], rs_recv.at[m, j - 1], peer(j),
        )

    def z_copy(m):
        return remote(x_out.at[m], x_in.at[m], z_send.at[m], z_recv.at[m], {"section": jnp.minimum(sec + 1, last)})

    def z_back(m):
        return remote(x_out.at[m], x_in.at[m], z_send.at[m], z_recv.at[m], {"section": jnp.maximum(sec - 1, 0)})

    def stage_a(m):
        @pl.when(sec > 0)
        def _():
            z_back(m).wait_recv()

        wide = x_in[m].astype(jnp.float32)
        scale = lax.rsqrt(jnp.mean(wide * wide, axis=-1, keepdims=True) + 1e-06)
        gathered[m, core, chip] = (wide * scale * gain[...]).astype(jnp.bfloat16)
        for j in range(1, chips):
            ag_copy(m, j, chip).start()

    def stage_f(m):
        for j in range(1, chips):
            ag_copy(m, j, lax.rem(chip + chips - j, chips)).wait_recv()
        fw_copy(m, core).start()

    def stage_b(m):
        fw_copy(m, other).wait_recv()
        piece = gathered[m].reshape(groups * block, width)
        for at, size in chunks(ff, 256):
            gate = jnp.dot(piece, wg[:, at:at + size], preferred_element_type=jnp.float32)
            upper = jnp.dot(piece, wu[:, at:at + size], preferred_element_type=jnp.float32)
            hidden[:, at:at + size] = (gate / (1.0 + jnp.exp(-gate)) * upper).astype(jnp.bfloat16)
        units = hidden[...]
        for at, size in chunks(width, 256):
            down = jnp.dot(units, wd[:, at:at + size], preferred_element_type=jnp.float32)
            part[m, :, :, :, at:at + size] = down.astype(jnp.bfloat16).reshape(2, chips, block, size)
        pr_copy(m).start()

    def stage_r(m):
        pr_copy(m).wait_recv()
        both = part[m, core].astype(jnp.float32) + part_in[m].astype(jnp.float32)
        paired[m] = both.astype(jnp.bfloat16)
        for j in range(1, chips):
            rs_copy(m, j).start()

    def stage_c(m):
        total = x_in[m].astype(jnp.float32) + paired[m, chip].astype(jnp.float32)
        for j in range(1, chips):
            rs_copy(m, j).wait_recv()
            total = total + paired_in[m, j - 1].astype(jnp.float32)
        state = total.astype(jnp.bfloat16)
        x_out[m] = state

        @pl.when(sec < last)
        def _():
            z_copy(m).start()

        @pl.when(sec == last)
        def _():
            wide = state.astype(jnp.float32)
            scale = lax.rsqrt(jnp.mean(wide * wide, axis=-1, keepdims=True) + 1e-06)
            value = jnp.sum(wide * scale * final_gain[...] * head[...], axis=-1, keepdims=True)
            reward_cols[m] = jnp.broadcast_to(value, (block, LANES))

    stage_a(0)
    for j in range(1, groups):
        to_group(marks, mk_send, mk_recv, j).start()
    stage_f(0)
    for load in loads:
        load.wait()

    def step(t, carry):
        @pl.when(t + 1 < MICRO)
        def _():
            stage_a(t + 1)

        @pl.when(t < MICRO)
        def _():
            stage_b(t)

        @pl.when(t >= 1)
        def _():
            stage_c(t - 1)

        @pl.when(t < MICRO)
        def _():
            stage_r(t)

        @pl.when(t + 1 < MICRO)
        def _():
            stage_f(t + 1)

        return carry

    lax.fori_loop(0, MICRO + 1, step, 0)

    for j in range(1, groups):
        from_group(marks, mk_send, mk_recv, j).wait_recv()
    for r in range(groups):
        marks_wide[r] = jnp.transpose(jnp.broadcast_to(marks[r], (LANES, rows)))

    def up_copy(j):
        return remote(result.at[me], result.at[me], up_send.at[j - 1], up_recv.at[0], {"section": last - j})

    @pl.when(sec == last)
    def _():
        square = reward_cols[...].reshape(rows, LANES)
        on_line = lax.broadcasted_iota(jnp.int32, (rows, rows), 0) == lax.broadcasted_iota(jnp.int32, (rows, rows), 1)
        row = jnp.sum(jnp.where(on_line, square, 0.0), axis=0, keepdims=True)
        priority = jnp.exp(0.6 * jnp.log(jnp.abs(row - returns[...]) + 0.05))
        result[me, 0:1] = row
        result[me, 1:2] = priority
        for j in range(1, sections):
            up_copy(j).start()

    @pl.when(sec < last)
    def _():
        up_copy(1).wait_recv()

    for j in range(1, groups):
        to_group(result, rw_send, rw_recv, j).start()

    mine = result[me, 0:1]
    share = rows // sections
    picked = mine[:, 0:share]
    for s in range(1, sections):
        picked = jnp.where(sec == s, mine[:, s * share:(s + 1) * share], picked)
    rewards_out[...] = picked

    for j in range(1, groups):
        from_group(result, rw_send, rw_recv, j).wait_recv()
    for r in range(groups):
        prio_wide[r] = jnp.transpose(jnp.broadcast_to(result[r, 1:2], (LANES, rows)))

    lines = old.shape[0]
    table = lines * LANES
    batch = 4
    lane = lax.broadcasted_iota(jnp.int32, (1, LANES), 1).astype(jnp.float32)

    def match(g, carry):
        first = (me * table + g * (batch * LANES)).astype(jnp.float32)
        names = [first + (q * LANES) + lane for q in range(batch)]

        def one(r, best):
            best = list(best)
            for i in range(0, rows, 8):
                mark = marks_wide[r, i:i + 8, :]
                prio = prio_wide[r, i:i + 8, :]
                for q in range(batch):
                    best[q] = jnp.maximum(best[q], jnp.where(mark == names[q], prio, 0.0))
            return tuple(best)

        best = lax.fori_loop(0, groups, one, tuple(jnp.zeros((8, LANES), jnp.float32) for _ in range(batch)))
        for q in range(batch):
            top = jnp.max(best[q], axis=0, keepdims=True)
            at = pl.ds(g * batch + q, 1)
            refreshed[at, :] = jnp.where(top > 0.0, top, old[at, :])
        return carry

    lax.fori_loop(0, lines // batch, match, 0)
    subtotal = jnp.sum(jnp.sum(refreshed[...], axis=0, keepdims=True), axis=1, keepdims=True)
    sums[me] = jnp.broadcast_to(subtotal, (1, LANES))
    for j in range(1, groups):
        to_group(sums, sm_send, sm_recv, j).start()

    for m in range(MICRO):
        for j in range(1, chips):
            ag_copy(m, j, chip).wait_send()
            rs_copy(m, j).wait_send()
        fw_copy(m, core).wait_send()
        pr_copy(m).wait_send()

    @pl.when(sec < last)
    def _():
        for m in range(MICRO):
            z_copy(m).wait_send()

    @pl.when(sec == last)
    def _():
        for j in range(1, sections):
            up_copy(j).wait_send()

    for j in range(1, groups):
        to_group(marks, mk_send, mk_recv, j).wait_send()
        to_group(result, rw_send, rw_recv, j).wait_send()

    for j in range(1, groups):
        from_group(sums, sm_send, sm_recv, j).wait_recv()
    total = sums[0]
    for r in range(1, groups):
        total = total + sums[r]
    tall = lines // sections
    weights_out[...] = refreshed[pl.ds(sec * tall, tall), :] * (table * groups / total)
    for j in range(1, groups):
        to_group(sums, sm_send, sm_recv, j).wait_send()


def on_device(
    features, ages, age_table, returns, owners, slots, norm_gain,
    w_gate, w_up, w_down, final_gain, reward_head, old_priority,
):
    sections, groups = lax.axis_size("section"), lax.axis_size("rows")
    rows, width = features.shape
    block = rows // MICRO
    chips = groups // 2
    ff = w_gate.shape[2]
    table = old_priority.shape[0]
    lines = table // LANES
    target = (owners[:, 0] * table + slots).astype(jnp.float32).reshape(1, rows)
    vmem = pl.BlockSpec(memory_space=pltpu.VMEM)
    far = pl.BlockSpec(memory_space=pl.ANY)
    bf16, f32, dma = jnp.bfloat16, jnp.float32, pltpu.SemaphoreType.DMA
    rewards, weights = pl.pallas_call(
        functools.partial(kernel, sections, groups),
        out_shape=(
            jax.ShapeDtypeStruct((1, rows // sections), f32),
            jax.ShapeDtypeStruct((lines // sections, LANES), f32),
        ),
        in_specs=[vmem] * 6 + [far] * 3 + [vmem] * 3,
        out_specs=(vmem, vmem),
        scratch_shapes=[
            pltpu.VMEM((width, ff), bf16),
            pltpu.VMEM((width, ff), bf16),
            pltpu.VMEM((ff, width), bf16),
            pltpu.VMEM((MICRO, block, width), bf16),
            pltpu.VMEM((MICRO, block, width), bf16),
            pltpu.VMEM((MICRO, 2, chips, block, width), bf16),
            pltpu.VMEM((groups * block, ff), bf16),
            pltpu.VMEM((MICRO, 2, chips, block, width), bf16),
            pltpu.VMEM((MICRO, chips, block, width), bf16),
            pltpu.VMEM((MICRO, chips, block, width), bf16),
            pltpu.VMEM((MICRO, chips - 1, block, width), bf16),
            pltpu.VMEM((MICRO, block, LANES), f32),
            pltpu.VMEM((groups, 1, rows), f32),
            pltpu.VMEM((groups, rows, LANES), f32),
            pltpu.VMEM((groups, 2, rows), f32),
            pltpu.VMEM((groups, rows, LANES), f32),
            pltpu.VMEM((lines, LANES), f32),
            pltpu.VMEM((groups, 1, LANES), f32),
            dma((3,)),
            dma((MICRO, chips - 1)), dma((MICRO, chips - 1)),
            dma((MICRO,)), dma((MICRO,)),
            dma((MICRO,)), dma((MICRO,)),
            dma((MICRO, chips - 1)), dma((MICRO, chips - 1)),
            dma((MICRO,)), dma((MICRO,)),
            dma((groups,)), dma((groups,)),
            dma((sections - 1,)), dma((1,)),
            dma((groups,)), dma((groups,)),
            dma((groups,)), dma((groups,)),
        ],
        compiler_params=pltpu.CompilerParams(
            collective_id=0, has_side_effects=True, vmem_limit_bytes=56 * 1024 * 1024
        ),
        name="refresh",
    )(
        features, ages.reshape(1, rows), age_table, returns.reshape(1, rows), target,
        norm_gain, w_gate[0], w_up[0], w_down[0],
        final_gain.reshape(1, width), reward_head.reshape(1, width),
        old_priority.reshape(lines, LANES),
    )
    return rewards.reshape(-1), weights.reshape(-1)


def solution(mesh):
    placed = (
        P("rows", None),
        P("rows"),
        P(),
        P("rows"),
        P("rows", None),
        P("rows"),
        P("section", None),
        P("section", None, "rows"),
        P("section", None, "rows"),
        P("section", "rows", None),
        P(),
        P(),
        P("rows"),
    )
    return jax.shard_map(
        on_device,
        mesh=mesh,
        in_specs=placed,
        out_specs=(P(("rows", "section")), P(("rows", "section"))),
        check_vma=False,
    )
```

```python
import functools

import jax
import jax.numpy as jnp
from jax import lax
from jax.experimental import pallas as pl
from jax.experimental.pallas import tpu as pltpu
from jax.sharding import PartitionSpec as P

MICRO = 8
MESH = pl.DeviceIdType.MESH
LANES = 128


def chunks(total, size):
    return [(at, min(size, total - at)) for at in range(0, total, size)]


def flipped(index, mask):
    moved, bit = index, 1
    while bit <= mask:
        if mask & bit:
            moved = moved + bit * (1 - 2 * lax.rem(index // bit, 2))
        bit *= 2
    return moved


def remote(src, dst, send_sem, recv_sem, where):
    return pltpu.make_async_remote_copy(
        src_ref=src, dst_ref=dst, send_sem=send_sem, recv_sem=recv_sem,
        device_id=where, device_id_type=MESH,
    )


def kernel(
    sections, groups,
    features, ages, age_table, returns, owners, slots, gain, w_gate, w_up, w_down,
    final_gain, head, old,
    rewards_out, weights_out,
    wg, wu, wd, wg_up, wu_up, x_in, x_out, gathered, hidden, part, part_in, paired, paired_in,
    final_row, reward_cols, marks, marks_wide, result, prio_wide, refreshed, sums,
    w_sem,
    ag_send, ag_recv, fw_send, fw_recv, pr_send, pr_recv, rs_send, rs_recv, z_send, z_recv,
    mk_send, mk_recv, up_send, up_recv, rw_send, rw_recv, sm_send, sm_recv,
):
    sec = lax.axis_index("section")
    me = lax.axis_index("rows")
    chips = groups // 2
    chip, core = me // 2, lax.rem(me, 2)
    other = 1 - core
    sibling = chip * 2 + other
    far_first = sorted(range(1, chips), key=lambda j: (-j.bit_count(), j))
    block, width = x_in.shape[1], x_in.shape[2]
    rows = x_in.shape[0] * block
    ff = hidden.shape[1]
    last = sections - 1

    loads = [
        pltpu.make_async_copy(w_gate, wg, w_sem.at[0]),
        pltpu.make_async_copy(w_up, wu, w_sem.at[1]),
        pltpu.make_async_copy(w_down, wd, w_sem.at[2]),
    ]
    loads[0].start()
    loads[1].start()

    barrier = pltpu.get_barrier_semaphore()
    for j in range(1, groups):
        pl.semaphore_signal(barrier, inc=1, device_id={"rows": lax.rem(me + j, groups)}, device_id_type=MESH)
    for j in range(1, sections):
        pl.semaphore_signal(barrier, inc=1, device_id={"section": lax.rem(sec + j, sections)}, device_id_type=MESH)

    marks[me] = (owners[...] * (old.shape[0] * LANES) + slots[...]).astype(jnp.float32)

    for i in range(final_gain.shape[0]):
        final_row[0:1, i * LANES:(i + 1) * LANES] = final_gain[i:i + 1, :]
        final_row[1:2, i * LANES:(i + 1) * LANES] = head[i:i + 1, :]

    @pl.when(sec == 0)
    def _():
        tall = jnp.transpose(jnp.broadcast_to(ages[...].astype(jnp.float32), (LANES, rows)))
        buckets = age_table.shape[0]
        onehot = (
            tall[:, :buckets] == lax.broadcasted_iota(jnp.int32, (rows, buckets), 1).astype(jnp.float32)
        ).astype(jnp.float32).astype(jnp.bfloat16)
        for at, size in chunks(width, 512):
            entry = features[:, at:at + size].astype(jnp.float32) + jnp.dot(
                onehot, age_table[:, at:at + size], preferred_element_type=jnp.float32
            )
            x_in[:, :, at:at + size] = entry.astype(jnp.bfloat16).reshape(MICRO, block, size)

    pl.semaphore_wait(barrier, groups - 1 + sections - 1)

    def to_group(ref, send, recv, j):
        return remote(ref.at[me], ref.at[me], send.at[j], recv.at[j], {"rows": lax.rem(me + j, groups)})

    def from_group(ref, send, recv, j):
        spot = ref.at[lax.rem(me + groups - j, groups)]
        return remote(spot, spot, send.at[j], recv.at[j], {"rows": lax.rem(me + j, groups)})

    def peer(j):
        return {"rows": flipped(chip, j) * 2 + core}

    def ag_copy(m, j, spot):
        block_ref = gathered.at[m, core, spot]
        return remote(block_ref, block_ref, ag_send.at[m, j - 1], ag_recv.at[m, j - 1], peer(j))

    def fw_copy(m, half):
        half_ref = gathered.at[m, half]
        return remote(half_ref, half_ref, fw_send.at[m], fw_recv.at[m], {"rows": sibling})

    def pr_copy(m):
        return remote(part.at[m, other], part_in.at[m], pr_send.at[m], pr_recv.at[m], {"rows": sibling})

    def rs_copy(m, j):
        return remote(
            paired.at[m, flipped(chip, j)], paired_in.at[m, j - 1],
            rs_send.at[m, j - 1], rs_recv.at[m, j - 1], peer(j),
        )

    def z_copy(m):
        return remote(x_out.at[m], x_in.at[m], z_send.at[m], z_recv.at[m], {"section": jnp.minimum(sec + 1, last)})

    def z_back(m):
        return remote(x_out.at[m], x_in.at[m], z_send.at[m], z_recv.at[m], {"section": jnp.maximum(sec - 1, 0)})

    def stage_a(m):
        @pl.when(sec > 0)
        def _():
            z_back(m).wait_recv()

        wide = x_in[m].astype(jnp.float32)
        scale = lax.rsqrt(jnp.mean(wide * wide, axis=-1, keepdims=True) + 1e-06)
        gathered[m, core, chip] = (wide * scale * gain[...]).astype(jnp.bfloat16)
        for j in far_first:
            ag_copy(m, j, chip).start()

    def stage_f(m):
        for j in far_first:
            ag_copy(m, j, flipped(chip, j)).wait_recv()
        fw_copy(m, core).start()

    def stage_b(m):
        fw_copy(m, other).wait_recv()
        piece = gathered[m].reshape(groups * block, width)
        for at, size in chunks(ff, 256):
            gate = jnp.dot(piece, wg_up[:, at:at + size], preferred_element_type=jnp.float32)
            upper = jnp.dot(piece, wu_up[:, at:at + size], preferred_element_type=jnp.float32)
            hidden[:, at:at + size] = (gate / (1.0 + jnp.exp(-gate)) * upper).astype(jnp.bfloat16)
        units = hidden[...]
        for at, size in chunks(width, 256):
            down = jnp.dot(units, wd[:, at:at + size], preferred_element_type=jnp.float32)
            part[m, :, :, :, at:at + size] = down.astype(jnp.bfloat16).reshape(2, chips, block, size)
        pr_copy(m).start()

    def stage_r(m):
        pr_copy(m).wait_recv()
        both = part[m, core].astype(jnp.float32) + part_in[m].astype(jnp.float32)
        paired[m] = both.astype(jnp.bfloat16)
        for j in far_first:
            rs_copy(m, j).start()

    def stage_c(m):
        total = x_in[m].astype(jnp.float32) + paired[m, chip].astype(jnp.float32)
        for j in far_first:
            rs_copy(m, j).wait_recv()
            total = total + paired_in[m, j - 1].astype(jnp.float32)
        state = total.astype(jnp.bfloat16)
        x_out[m] = state

        @pl.when(sec < last)
        def _():
            z_copy(m).start()

        @pl.when(sec == last)
        def _():
            wide = state.astype(jnp.float32)
            scale = lax.rsqrt(jnp.mean(wide * wide, axis=-1, keepdims=True) + 1e-06)
            value = jnp.sum(wide * scale * final_row[0:1] * final_row[1:2], axis=-1, keepdims=True)
            reward_cols[m] = jnp.broadcast_to(value, (block, LANES))

    stage_a(0)
    for j in range(1, groups):
        to_group(marks, mk_send, mk_recv, j).start()
    for load, flat, tall in ((loads[0], wg, wg_up), (loads[1], wu, wu_up)):
        load.wait()
        if load is loads[0]:
            loads[2].start()
        for at, size in chunks(ff, 256):
            tall[:, at:at + size] = jnp.transpose(flat[at:at + size, :])
    stage_f(0)
    loads[2].wait()

    def step(t, carry):
        @pl.when(t + 1 < MICRO)
        def _():
            stage_a(t + 1)

        @pl.when(t < MICRO)
        def _():
            stage_b(t)

        @pl.when(t >= 1)
        def _():
            stage_c(t - 1)

        @pl.when(t < MICRO)
        def _():
            stage_r(t)

        @pl.when(t + 1 < MICRO)
        def _():
            stage_f(t + 1)

        return carry

    lax.fori_loop(0, MICRO + 1, step, 0)

    for j in range(1, groups):
        from_group(marks, mk_send, mk_recv, j).wait_recv()
    for r in range(groups):
        marks_wide[r] = jnp.transpose(jnp.broadcast_to(marks[r], (LANES, rows)))

    def up_copy(j):
        return remote(result.at[me], result.at[me], up_send.at[j - 1], up_recv.at[0], {"section": last - j})

    @pl.when(sec == last)
    def _():
        square = reward_cols[...].reshape(rows, LANES)
        on_line = lax.broadcasted_iota(jnp.int32, (rows, rows), 0) == lax.broadcasted_iota(jnp.int32, (rows, rows), 1)
        row = jnp.sum(jnp.where(on_line, square, 0.0), axis=0, keepdims=True)
        priority = jnp.exp(0.6 * jnp.log(jnp.abs(row - returns[...]) + 0.05))
        result[me, 0:1] = row
        result[me, 1:2] = priority
        for j in range(1, sections):
            up_copy(j).start()

    @pl.when(sec < last)
    def _():
        up_copy(1).wait_recv()

    for j in range(1, groups):
        to_group(result, rw_send, rw_recv, j).start()

    mine = result[me, 0:1]
    share = rows // sections
    picked = mine[:, 0:share]
    for s in range(1, sections):
        picked = jnp.where(sec == s, mine[:, s * share:(s + 1) * share], picked)
    rewards_out[...] = picked

    for j in range(1, groups):
        from_group(result, rw_send, rw_recv, j).wait_recv()
    for r in range(groups):
        prio_wide[r] = jnp.transpose(jnp.broadcast_to(result[r, 1:2], (LANES, rows)))

    lines = old.shape[0]
    table = lines * LANES
    batch = 4
    lane = lax.broadcasted_iota(jnp.int32, (1, LANES), 1).astype(jnp.float32)

    def match(g, carry):
        first = (me * table + g * (batch * LANES)).astype(jnp.float32)
        names = [first + (q * LANES) + lane for q in range(batch)]

        def one(r, best):
            best = list(best)
            for i in range(0, rows, 8):
                mark = marks_wide[r, i:i + 8, :]
                prio = prio_wide[r, i:i + 8, :]
                for q in range(batch):
                    best[q] = jnp.maximum(best[q], jnp.where(mark == names[q], prio, 0.0))
            return tuple(best)

        best = lax.fori_loop(0, groups, one, tuple(jnp.zeros((8, LANES), jnp.float32) for _ in range(batch)))
        for q in range(batch):
            top = jnp.max(best[q], axis=0, keepdims=True)
            at = pl.ds(g * batch + q, 1)
            refreshed[at, :] = jnp.where(top > 0.0, top, old[at, :])
        return carry

    lax.fori_loop(0, lines // batch, match, 0)
    subtotal = jnp.sum(jnp.sum(refreshed[...], axis=0, keepdims=True), axis=1, keepdims=True)
    sums[me] = jnp.broadcast_to(subtotal, (1, LANES))
    for j in range(1, groups):
        to_group(sums, sm_send, sm_recv, j).start()

    for m in range(MICRO):
        for j in far_first:
            ag_copy(m, j, chip).wait_send()
            rs_copy(m, j).wait_send()
        fw_copy(m, core).wait_send()
        pr_copy(m).wait_send()

    @pl.when(sec < last)
    def _():
        for m in range(MICRO):
            z_copy(m).wait_send()

    @pl.when(sec == last)
    def _():
        for j in range(1, sections):
            up_copy(j).wait_send()

    for j in range(1, groups):
        to_group(marks, mk_send, mk_recv, j).wait_send()
        to_group(result, rw_send, rw_recv, j).wait_send()

    for j in range(1, groups):
        from_group(sums, sm_send, sm_recv, j).wait_recv()
    total = sums[0]
    for r in range(1, groups):
        total = total + sums[r]
    tall = lines // sections
    weights_out[...] = refreshed[pl.ds(sec * tall, tall), :] * (table * groups / total)
    for j in range(1, groups):
        to_group(sums, sm_send, sm_recv, j).wait_send()


def handed(rewards, weights, rewards_out, weights_out):
    rewards_out[...] = rewards[...]
    weights_out[...] = weights[...]


def on_device(
    features, ages, age_table, returns, owners, slots, norm_gain,
    w_gate, w_up, w_down, final_gain, reward_head, old_priority,
):
    sections, groups = lax.axis_size("section"), lax.axis_size("rows")
    rows, width = features.shape
    block = rows // MICRO
    chips = groups // 2
    ff = w_gate.shape[2]
    table = old_priority.shape[0]
    lines = table // LANES
    vmem = pl.BlockSpec(memory_space=pltpu.VMEM)
    far = pl.BlockSpec(memory_space=pl.ANY)
    bf16, f32, dma = jnp.bfloat16, jnp.float32, pltpu.SemaphoreType.DMA
    rewards, weights = pl.pallas_call(
        functools.partial(kernel, sections, groups),
        out_shape=(
            jax.ShapeDtypeStruct((1, rows // sections), f32),
            jax.ShapeDtypeStruct((lines // sections, LANES), f32),
        ),
        in_specs=[vmem] * 7 + [far] * 3 + [vmem] * 3,
        out_specs=(vmem, vmem),
        scratch_shapes=[
            pltpu.VMEM((ff, width), bf16),
            pltpu.VMEM((ff, width), bf16),
            pltpu.VMEM((ff, width), bf16),
            pltpu.VMEM((width, ff), bf16),
            pltpu.VMEM((width, ff), bf16),
            pltpu.VMEM((MICRO, block, width), bf16),
            pltpu.VMEM((MICRO, block, width), bf16),
            pltpu.VMEM((MICRO, 2, chips, block, width), bf16),
            pltpu.VMEM((groups * block, ff), bf16),
            pltpu.VMEM((MICRO, 2, chips, block, width), bf16),
            pltpu.VMEM((MICRO, chips, block, width), bf16),
            pltpu.VMEM((MICRO, chips, block, width), bf16),
            pltpu.VMEM((MICRO, chips - 1, block, width), bf16),
            pltpu.VMEM((2, width), f32),
            pltpu.VMEM((MICRO, block, LANES), f32),
            pltpu.VMEM((groups, 1, rows), f32),
            pltpu.VMEM((groups, rows, LANES), f32),
            pltpu.VMEM((groups, 2, rows), f32),
            pltpu.VMEM((groups, rows, LANES), f32),
            pltpu.VMEM((lines, LANES), f32),
            pltpu.VMEM((groups, 1, LANES), f32),
            dma((3,)),
            dma((MICRO, chips - 1)), dma((MICRO, chips - 1)),
            dma((MICRO,)), dma((MICRO,)),
            dma((MICRO,)), dma((MICRO,)),
            dma((MICRO, chips - 1)), dma((MICRO, chips - 1)),
            dma((MICRO,)), dma((MICRO,)),
            dma((groups,)), dma((groups,)),
            dma((sections - 1,)), dma((1,)),
            dma((groups,)), dma((groups,)),
            dma((groups,)), dma((groups,)),
        ],
        compiler_params=pltpu.CompilerParams(
            collective_id=0, has_side_effects=True, vmem_limit_bytes=56 * 1024 * 1024
        ),
        name="refresh",
    )(
        features, ages.reshape(1, rows), age_table, returns.reshape(1, rows),
        owners.reshape(1, rows), slots.reshape(1, rows),
        norm_gain, w_gate[0].T, w_up[0].T, w_down[0],
        final_gain.reshape(-1, LANES), reward_head.reshape(-1, LANES),
        old_priority.reshape(lines, LANES),
    )
    rewards, weights = pl.pallas_call(
        handed, out_shape=tuple(jax.ShapeDtypeStruct(each.shape, f32) for each in (rewards, weights)),
        in_specs=[vmem, vmem], out_specs=(vmem, vmem), name="handed",
    )(rewards, weights)
    return rewards.reshape(-1), weights.reshape(-1)


def solution(mesh):
    placed = (
        P("rows", None),
        P("rows"),
        P(),
        P("rows"),
        P("rows", None),
        P("rows"),
        P("section", None),
        P("section", None, "rows"),
        P("section", None, "rows"),
        P("section", "rows", None),
        P(),
        P(),
        P("rows"),
    )
    return jax.shard_map(
        on_device,
        mesh=mesh,
        in_specs=placed,
        out_specs=(P(("rows", "section")), P(("rows", "section"))),
        check_vma=False,
    )
```
